16 devices in a mesh: row: 2 (over z), col: 8 (over y, x, core).
Axes of the slice: x: 2, y: 2, z: 2, core: 2. Of those that a mesh axis runs over, the one named last changes fastest.
Arguments:
- w_in: float32 [2, 8, 3, 512, 1024], P('row', 'col')
- w_out: float32 [2, 8, 3, 1024, 512], P('row', 'col')
- inputs: bfloat16 [2, 8, 16, 512, 512], P('row', 'col')
- targets: bfloat16 [2, 8, 16, 512, 512], P('row', 'col')
Outputs:
- output 1: float32 [2, 8, 3, 512, 1024], P('row', 'col')
- output 2: float32 [2, 8, 3, 1024, 512], P('row', 'col')
All inputs are finite; a program needn't handle non-finite values.
Results may differ from the reference program's by a relative error of at most 0.00106204.
Values are sent between devices in bfloat16 or wider.
A program may use at most 1 GiB of HBM per device.

```python
import jax
import jax.numpy as jnp
from jax import lax

ROWS = 2
COLS = 8
LAYERS = 3
D = 512
FF = 1024
BATCH = 512
WINDOWS = 8

STEPS = 2 * WINDOWS
LEARN_RATE = 0.8 / LAYERS
EPS = 1e-6
INV_SQRT2 = 0.7071067811865476
INV_SQRT_2PI = 0.3989422804014327
SPREAD = 0.5
TARGET_SHIFT = 2.0


def setup_inputs(seed: int = 0) -> dict:
    key_list = jax.random.split(jax.random.key(seed), 8)
    norm_scale = (1.0 + SPREAD * SPREAD) ** -0.5
    shape_in = (ROWS, COLS, LAYERS, D, FF)
    shape_out = (ROWS, COLS, LAYERS, FF, D)
    data_shape = (ROWS, COLS, STEPS, BATCH, D)
    base_in = jax.random.normal(key_list[0], (LAYERS, D, FF), jnp.float32)
    base_out = jax.random.normal(key_list[1], (LAYERS, FF, D), jnp.float32)
    w_in = (base_in + SPREAD * jax.random.normal(key_list[2], shape_in, jnp.float32)) * (norm_scale * D ** -0.5)
    w_out = (base_out + SPREAD * jax.random.normal(key_list[3], shape_out, jnp.float32)) * (norm_scale * FF ** -0.5)
    shift_in = jax.random.normal(key_list[4], (ROWS, COLS, 1, 1, D), jnp.float32)
    shift_tgt = TARGET_SHIFT * jax.random.normal(key_list[5], (ROWS, COLS, 1, 1, D), jnp.float32)
    inputs = (jax.random.normal(key_list[6], data_shape, jnp.float32) + shift_in).astype(jnp.bfloat16)
    targets = (jax.random.normal(key_list[7], data_shape, jnp.float32) + shift_tgt).astype(jnp.bfloat16)
    return {"w_in": w_in, "w_out": w_out, "inputs": inputs, "targets": targets}


def rms_norm(rows):
    return rows * lax.rsqrt(jnp.mean(rows * rows, axis=-1, keepdims=True) + EPS)


def rms_back(rows, grad_norm):
    inv_rms = lax.rsqrt(jnp.mean(rows * rows, axis=-1, keepdims=True) + EPS)
    row_dot = jnp.mean(rows * grad_norm, axis=-1, keepdims=True)
    return inv_rms * grad_norm - rows * (inv_rms * inv_rms * inv_rms) * row_dot


def gelu_exact(pre_act):
    return 0.5 * pre_act * (1.0 + lax.erf(pre_act * INV_SQRT2))


def gelu_slope(pre_act):
    return 0.5 * (1.0 + lax.erf(pre_act * INV_SQRT2)) + pre_act * jnp.exp(-0.5 * pre_act * pre_act) * INV_SQRT_2PI


def device_grads(w_in, w_out, rows_in, rows_tgt):
    hidden = rows_in
    saved_acts = []
    for layer_idx in range(LAYERS):
        w1_bf = w_in[layer_idx].astype(jnp.bfloat16)
        w2_bf = w_out[layer_idx].astype(jnp.bfloat16)
        h_f32 = hidden.astype(jnp.float32)
        normed = rms_norm(h_f32).astype(jnp.bfloat16)
        pre_act = jnp.dot(normed, w1_bf, preferred_element_type=jnp.float32)
        act_bf = gelu_exact(pre_act).astype(jnp.bfloat16)
        hidden = (h_f32 + jnp.dot(act_bf, w2_bf, preferred_element_type=jnp.float32)).astype(jnp.bfloat16)
        saved_acts.append((w1_bf, w2_bf, h_f32, normed, pre_act, act_bf))
    grad_h = (hidden.astype(jnp.float32) - rows_tgt.astype(jnp.float32)) * (2.0 / (BATCH * D))
    grads_in = [None] * LAYERS
    grads_out = [None] * LAYERS
    for layer_idx in reversed(range(LAYERS)):
        w1_bf, w2_bf, h_f32, normed, pre_act, act_bf = saved_acts[layer_idx]
        grad_bf = grad_h.astype(jnp.bfloat16)
        grads_out[layer_idx] = jnp.dot(act_bf.T, grad_bf, preferred_element_type=jnp.float32)
        d_pre = (jnp.dot(grad_bf, w2_bf.T, preferred_element_type=jnp.float32) * gelu_slope(pre_act)).astype(jnp.bfloat16)
        grads_in[layer_idx] = jnp.dot(normed.T, d_pre, preferred_element_type=jnp.float32)
        if layer_idx > 0:
            grad_h = grad_h + rms_back(h_f32, jnp.dot(d_pre, w1_bf.T, preferred_element_type=jnp.float32))
    return jnp.stack(grads_in), jnp.stack(grads_out)


def all_grads(w_in, w_out, rows_in, rows_tgt):
    dev_count = ROWS * COLS

    def one_device(operands):
        return device_grads(operands[0], operands[1], operands[2], operands[3])

    grads_in, grads_out = lax.map(one_device, (
        w_in.reshape((dev_count,) + w_in.shape[2:]),
        w_out.reshape((dev_count,) + w_out.shape[2:]),
        rows_in.reshape((dev_count,) + rows_in.shape[2:]),
        rows_tgt.reshape((dev_count,) + rows_tgt.shape[2:])))
    return grads_in.reshape(w_in.shape), grads_out.reshape(w_out.shape)


def neighbour_mix(params):
    wire_copy = params.astype(jnp.bfloat16)
    mix_sum = params + jnp.roll(wire_copy, 1, axis=1).astype(jnp.float32)
    mix_sum = mix_sum + jnp.roll(wire_copy, -1, axis=1).astype(jnp.float32)
    mix_sum = mix_sum + jnp.roll(wire_copy, 1, axis=0).astype(jnp.float32)
    mix_sum = mix_sum + jnp.roll(wire_copy, -1, axis=0).astype(jnp.float32)
    return mix_sum / 5.0


def reference(w_in, w_out, inputs, targets):
    def window_body(carry, window_idx):
        cur_in, cur_out = carry
        step_a = 2 * window_idx
        rows_a = lax.dynamic_index_in_dim(inputs, step_a, axis=2, keepdims=False)
        tgt_a = lax.dynamic_index_in_dim(targets, step_a, axis=2, keepdims=False)
        rows_b = lax.dynamic_index_in_dim(inputs, step_a + 1, axis=2, keepdims=False)
        tgt_b = lax.dynamic_index_in_dim(targets, step_a + 1, axis=2, keepdims=False)
        g_a_in, g_a_out = all_grads(cur_in, cur_out, rows_a, tgt_a)
        g_b_in, g_b_out = all_grads(cur_in - LEARN_RATE * g_a_in, cur_out - LEARN_RATE * g_a_out, rows_b, tgt_b)
        new_in = neighbour_mix(cur_in) - LEARN_RATE * (g_a_in + g_b_in)
        new_out = neighbour_mix(cur_out) - LEARN_RATE * (g_a_out + g_b_out)
        return (new_in, new_out), None

    final_pair = lax.scan(window_body, (w_in, w_out), jnp.arange(WINDOWS))[0]
    return final_pair[0], final_pair[1]
```

```python
import jax
import jax.numpy as jnp
from jax import lax
from jax.experimental import pallas as pl
from jax.experimental.pallas import tpu as pltpu
from jax.sharding import PartitionSpec as P

LR_SCALE = 0.8
EPS = 1e-6
INV_SQRT2 = 0.7071067811865476
INV_SQRT_2PI = 0.3989422804014327
CONTRACT_ROWS = (((0,), (0,)), ((), ()))
CONTRACT_LAST = (((1,), (1,)), ((), ()))
MESH = pl.DeviceIdType.MESH
F32 = jnp.float32
BF16 = jnp.bfloat16

PARTS = 4
ROW_BLOCK = 256


def solution(mesh):
    col_size = mesh.shape["col"]

    def device_kernel(w1_hbm, w2_hbm, a_hbm, t_hbm, out1, out2, got1, got2,
                      p1, p2, sum1, sum2, pb1, pb2, qb1, qb2,
                      hid, normed, slope, act, grad_h, grad_bf, d_pre, rows_buf, tgt_buf, stage1, stage2,
                      load_sem, data_sem, stage_sem, send_sem, recv_sem):
        layers, dim, ff = p1.shape
        batch = rows_buf.shape[1]
        steps = a_hbm.shape[0]
        windows = steps // 2
        learn_rate = LR_SCALE / layers
        rows1, rows2 = dim // PARTS, ff // PARTS
        pieces = layers * PARTS

        row = lax.axis_index("row")
        col = lax.axis_index("col")
        targets = [(row, lax.rem(col + 1, col_size)), (row, lax.rem(col + col_size - 1, col_size)), (1 - row, col)]

        def piece(idx):
            layer = idx // PARTS
            part = lax.rem(idx, PARTS)
            at1 = (layer, pl.ds(pl.multiple_of(part * rows1, rows1), rows1))
            at2 = (layer, pl.ds(pl.multiple_of(part * rows2, rows2), rows2))
            return at1, at2

        def sends(idx, slot):
            at1, at2 = piece(idx)
            copies = []
            for k, target in enumerate(targets):
                for which, (src, dst, at) in enumerate(((pb1, got1, at1), (pb2, got2, at2))):
                    copies.append(pltpu.make_async_remote_copy(
                        src_ref=src.at[at], dst_ref=dst.at[(slot, k) + at],
                        send_sem=send_sem.at[idx, which, k], recv_sem=recv_sem.at[slot, idx, which, k],
                        device_id=target, device_id_type=MESH))
            return copies

        def loads(idx):
            at1, at2 = piece(idx)
            return [pltpu.make_async_copy(w1_hbm.at[at1], p1.at[at1], load_sem.at[idx, 0]),
                    pltpu.make_async_copy(w2_hbm.at[at2], p2.at[at2], load_sem.at[idx, 1])]

        def stores(idx):
            at1, at2 = piece(idx)
            return [pltpu.make_async_copy(p1.at[at1], out1.at[at1], load_sem.at[idx, 0]),
                    pltpu.make_async_copy(p2.at[at2], out2.at[at2], load_sem.at[idx, 1])]

        def fetch(step):
            slot = lax.rem(step, 2)
            return [pltpu.make_async_copy(a_hbm.at[step], rows_buf.at[slot], data_sem.at[slot, 0]),
                    pltpu.make_async_copy(t_hbm.at[step], tgt_buf.at[slot], data_sem.at[slot, 1])]

        def start_all(copies):
            for copy in copies:
                copy.start()

        def wait_all(copies):
            for copy in copies:
                copy.wait()

        def load_one(idx, carry):
            start_all(loads(idx))
            return carry
        lax.fori_loop(0, pieces, load_one, 0)
        start_all(fetch(0))

        barrier = pltpu.get_barrier_semaphore()
        for target in targets:
            pl.semaphore_signal(barrier, inc=1, device_id=target, device_id_type=MESH)
        pl.semaphore_wait(barrier, len(targets))

        def first_send(idx, carry):
            wait_all(loads(idx))
            at1, at2 = piece(idx)
            pb1[at1] = p1[at1].astype(BF16)
            pb2[at2] = p2[at2].astype(BF16)
            start_all(sends(idx, 0))
            return carry
        lax.fori_loop(0, pieces, first_send, 0)

        def local_step(step, first, wb1, wb2):
            slot = 0 if first else 1
            wait_all(fetch(step))
            @pl.when(step + 1 < steps)
            def _():
                start_all(fetch(step + 1))

            def rms_rows(src, layer):
                def body(i, carry):
                    at = pl.ds(pl.multiple_of(i * 32, 32), 32)
                    v = src[at].astype(F32)
                    normed[layer, at] = (v * lax.rsqrt(jnp.mean(v * v, axis=-1, keepdims=True) + EPS)).astype(BF16)
                    return carry
                lax.fori_loop(0, batch // 32, body, 0)

            def forward(layer, h_in, h_out):
                rms_rows(h_in, layer)
                for blk in range(batch // ROW_BLOCK):
                    rows = pl.ds(blk * ROW_BLOCK, ROW_BLOCK)
                    slope[layer, rows] = jnp.dot(normed[layer, rows], wb1[layer], preferred_element_type=F32)

                    def gelu(i, carry):
                        at = pl.ds(pl.multiple_of(blk * ROW_BLOCK + i * 16, 16), 16)
                        for half in range(2):
                            lanes = pl.ds(half * (ff // 2), ff // 2)
                            z = slope[layer, at, lanes]
                            phi = 0.5 * (1.0 + lax.erf(z * INV_SQRT2))
                            act[layer, at, lanes] = (z * phi).astype(BF16)
                            slope[layer, at, lanes] = phi + z * jnp.exp(-0.5 * z * z) * INV_SQRT_2PI
                        return carry
                    lax.fori_loop(0, ROW_BLOCK // 16, gelu, 0)
                    h_out[rows] = (h_in[rows].astype(F32) + jnp.dot(act[layer, rows], wb2[layer], preferred_element_type=F32)).astype(BF16)

            forward(0, rows_buf.at[slot], hid.at[0])

            def forward_rest(layer, carry):
                forward(layer, hid.at[layer - 1], hid.at[layer])
                return carry
            lax.fori_loop(1, layers, forward_rest, 0)

            def loss(i, carry):
                at = pl.ds(pl.multiple_of(i * 32, 32), 32)
                e = (hid[layers - 1, at].astype(F32) - tgt_buf[slot, at].astype(F32)) * (2.0 / (batch * dim))
                grad_h[at] = e
                grad_bf[at] = e.astype(BF16)
                return carry
            lax.fori_loop(0, batch // 32, loss, 0)

            def apply(p, total, qb, layer, at, grad):
                if first:
                    total[layer, at] = grad
                    qb[layer, at] = (p[layer, at] - learn_rate * grad).astype(BF16)
                else:
                    total[layer, at] = learn_rate * (total[layer, at] + grad)

            def backward(back, carry):
                layer = layers - 1 - back
                for tile in range(ff // 256):
                    at = pl.ds(tile * 256, 256)
                    apply(p2, sum2, qb2, layer, at,
                          lax.dot_general(act[layer, :, at], grad_bf[...], CONTRACT_ROWS, preferred_element_type=F32))
                for blk in range(batch // ROW_BLOCK):
                    rows = pl.ds(blk * ROW_BLOCK, ROW_BLOCK)
                    d_pre[rows] = (lax.dot_general(grad_bf[rows], wb2[layer], CONTRACT_LAST, preferred_element_type=F32)
                                   * slope[layer, rows]).astype(BF16)
                for tile in range(dim // 128):
                    at = pl.ds(tile * 128, 128)
                    apply(p1, sum1, qb1, layer, at,
                          lax.dot_general(normed[layer, :, at], d_pre[...], CONTRACT_ROWS, preferred_element_type=F32))

                @pl.when(layer > 0)
                def _():
                    h_in = hid.at[layer - 1]
                    for blk in range(batch // ROW_BLOCK):
                        rows = pl.ds(blk * ROW_BLOCK, ROW_BLOCK)
                        grad_norm = lax.dot_general(d_pre[rows], wb1[layer], CONTRACT_LAST, preferred_element_type=F32)
                        h = h_in[rows].astype(F32)
                        inv_rms = lax.rsqrt(jnp.mean(h * h, axis=-1, keepdims=True) + EPS)
                        row_dot = jnp.mean(h * grad_norm, axis=-1, keepdims=True)
                        e = grad_h[rows] + (inv_rms * grad_norm - h * (inv_rms * inv_rms * inv_rms) * row_dot)
                        grad_h[rows] = e
                        grad_bf[rows] = e.astype(BF16)
                return carry
            lax.fori_loop(0, layers, backward, 0)

        def mix(window):
            slot = lax.rem(window, 2)

            def one(idx, carry):
                at1, at2 = piece(idx)
                wait_all(sends(idx, slot))
                staged = []
                for k in range(len(targets)):
                    staged.append(pltpu.make_async_copy(got1.at[(slot, k) + at1], stage1.at[k], stage_sem.at[0, k]))
                    staged.append(pltpu.make_async_copy(got2.at[(slot, k) + at2], stage2.at[k], stage_sem.at[1, k]))
                start_all(staged)
                wait_all(staged)
                for p, pb, total, stage, (layer, span) in ((p1, pb1, sum1, stage1, at1), (p2, pb2, sum2, stage2, at2)):
                    rows = stage.shape[1]
                    base = lax.rem(idx, PARTS) * rows

                    def some(i, inner):
                        src = pl.ds(pl.multiple_of(i * 16, 16), 16)
                        at = (layer, pl.ds(pl.multiple_of(base + i * 16, 16), 16))
                        acc = p[at] + stage[0, src].astype(F32)
                        acc = acc + stage[1, src].astype(F32)
                        other = stage[2, src].astype(F32)
                        acc = (acc + other) + other
                        new = acc / 5.0 - total[at]
                        p[at] = new
                        pb[at] = new.astype(BF16)
                        return inner
                    lax.fori_loop(0, rows // 16, some, 0)

                @pl.when(window + 1 < windows)
                def _():
                    start_all(sends(idx, 1 - slot))

                @pl.when(window + 1 == windows)
                def _():
                    start_all(stores(idx))
                return carry
            lax.fori_loop(0, pieces, one, 0)

        def one_window(window, carry):
            local_step(2 * window, True, pb1, pb2)
            local_step(2 * window + 1, False, qb1, qb2)
            mix(window)
            return carry
        lax.fori_loop(0, windows, one_window, 0)

        def finish(idx, carry):
            wait_all(stores(idx))
            return carry
        lax.fori_loop(0, pieces, finish, 0)

    def device_program(w_in, w_out, inputs, targets):
        layers, dim, ff = w_in.shape[2:]
        steps, batch = inputs.shape[2:4]
        pieces = layers * PARTS
        any_space = pl.BlockSpec(memory_space=pl.ANY)
        shape1, shape2 = (layers, dim, ff), (layers, ff, dim)
        sums = pl.pallas_call(
            device_kernel,
            out_shape=[jax.ShapeDtypeStruct(shape1, F32), jax.ShapeDtypeStruct(shape2, F32),
                       jax.ShapeDtypeStruct((2, 3) + shape1, BF16), jax.ShapeDtypeStruct((2, 3) + shape2, BF16)],
            in_specs=[any_space] * 4,
            out_specs=[any_space] * 4,
            scratch_shapes=[
                pltpu.VMEM(shape1, F32), pltpu.VMEM(shape2, F32),
                pltpu.VMEM(shape1, F32), pltpu.VMEM(shape2, F32),
                pltpu.VMEM(shape1, BF16), pltpu.VMEM(shape2, BF16),
                pltpu.VMEM(shape1, BF16), pltpu.VMEM(shape2, BF16),
                pltpu.VMEM((layers, batch, dim), BF16),
                pltpu.VMEM((layers, batch, dim), BF16),
                pltpu.VMEM((layers, batch, ff), F32),
                pltpu.VMEM((layers, batch, ff), BF16),
                pltpu.VMEM((batch, dim), F32),
                pltpu.VMEM((batch, dim), BF16),
                pltpu.VMEM((batch, ff), BF16),
                pltpu.VMEM((2, batch, dim), BF16), pltpu.VMEM((2, batch, dim), BF16),
                pltpu.VMEM((3, dim // PARTS, ff), BF16), pltpu.VMEM((3, ff // PARTS, dim), BF16),
                pltpu.SemaphoreType.DMA((pieces, 2)),
                pltpu.SemaphoreType.DMA((2, 2)),
                pltpu.SemaphoreType.DMA((2, 3)),
                pltpu.SemaphoreType.DMA((pieces, 2, 3)),
                pltpu.SemaphoreType.DMA((2, pieces, 2, 3)),
            ],
            compiler_params=pltpu.CompilerParams(collective_id=0, has_side_effects=True, vmem_limit_bytes=67043328),
        )(w_in[0, 0], w_out[0, 0], inputs[0, 0], targets[0, 0])
        return sums[0][None, None], sums[1][None, None]

    block_spec = P("row", "col")
    return jax.shard_map(device_program, mesh=mesh,
                         in_specs=(block_spec, block_spec, block_spec, block_spec),
                         out_specs=(block_spec, block_spec), check_vma=False)
```

```python
import jax
import jax.numpy as jnp
from jax import lax
from jax.experimental import pallas as pl
from jax.experimental.pallas import tpu as pltpu
from jax.sharding import PartitionSpec as P

LR_SCALE = 0.8
EPS = 1e-6
INV_SQRT2 = 0.7071067811865476
INV_SQRT_2PI = 0.3989422804014327
CONTRACT_ROWS = (((0,), (0,)), ((), ()))
CONTRACT_LAST = (((1,), (1,)), ((), ()))
MESH = pl.DeviceIdType.MESH
F32 = jnp.float32
BF16 = jnp.bfloat16

PARTS = 2
ROW_BLOCK = 256


def solution(mesh):
    col_size = mesh.shape["col"]

    def device_kernel(w1_hbm, w2_hbm, a_hbm, t_hbm, p1, p2, got1, got2,
                      sum1, sum2, pb1, pb2, qb1, qb2,
                      hid, normed, slope, act, grad_h, grad_bf, d_pre, rows_buf, tgt_buf, stage1, stage2,
                      load_sem, data_sem, stage_sem, send_sem, recv_sem):
        layers, dim, ff = p1.shape
        batch = rows_buf.shape[1]
        steps = a_hbm.shape[0]
        windows = steps // 2
        learn_rate = LR_SCALE / layers
        rows1, rows2 = dim // PARTS, ff // PARTS
        pieces = layers * PARTS

        row = lax.axis_index("row")
        col = lax.axis_index("col")
        targets = [(row, lax.rem(col + 1, col_size)), (row, lax.rem(col + col_size - 1, col_size)), (1 - row, col)]

        def piece(idx):
            layer = idx // PARTS
            part = lax.rem(idx, PARTS)
            at1 = (layer, pl.ds(pl.multiple_of(part * rows1, rows1), rows1))
            at2 = (layer, pl.ds(pl.multiple_of(part * rows2, rows2), rows2))
            return at1, at2

        def sends(idx, slot, which):
            src, dst = ((pb1, got1), (pb2, got2))[which]
            at = piece(idx)[which]
            return [pltpu.make_async_remote_copy(
                src_ref=src.at[at], dst_ref=dst.at[(slot, k) + at],
                send_sem=send_sem.at[idx, which, k], recv_sem=recv_sem.at[slot, idx, which, k],
                device_id=target, device_id_type=MESH) for k, target in enumerate(targets)]

        def loads(idx):
            at1, at2 = piece(idx)
            return [pltpu.make_async_copy(w1_hbm.at[at1], p1.at[at1], load_sem.at[idx, 0]),
                    pltpu.make_async_copy(w2_hbm.at[at2], p2.at[at2], load_sem.at[idx, 1])]

        def fetch(step):
            slot = lax.rem(step, 2)
            return [pltpu.make_async_copy(a_hbm.at[step], rows_buf.at[slot], data_sem.at[slot, 0]),
                    pltpu.make_async_copy(t_hbm.at[step], tgt_buf.at[slot], data_sem.at[slot, 1])]

        def start_all(copies):
            for copy in copies:
                copy.start()

        def wait_all(copies):
            for copy in copies:
                copy.wait()

        ahead = min(3, pieces)
        for idx in range(ahead):
            start_all(loads(idx))

        barrier = pltpu.get_barrier_semaphore()
        for target in targets:
            pl.semaphore_signal(barrier, inc=1, device_id=target, device_id_type=MESH)
        pl.semaphore_wait(barrier, len(targets))

        def first_send(idx, carry):
            for which, (load, p, pb) in enumerate(zip(loads(idx), (p1, p2), (pb1, pb2))):
                load.wait()
                at = piece(idx)[which]
                pb[at] = p[at].astype(BF16)
                start_all(sends(idx, 0, which))

            @pl.when(idx + ahead < pieces)
            def _():
                start_all(loads(idx + ahead))
            return carry
        lax.fori_loop(0, pieces, first_send, 0)
        start_all(fetch(0))

        def local_step(step, first, wb1, wb2):
            slot = 0 if first else 1
            wait_all(fetch(step))
            @pl.when(step + 1 < steps)
            def _():
                start_all(fetch(step + 1))

            def rms_rows(src, layer):
                def body(i, carry):
                    at = pl.ds(pl.multiple_of(i * 32, 32), 32)
                    v = src[at].astype(F32)
                    normed[layer, at] = (v * lax.rsqrt(jnp.mean(v * v, axis=-1, keepdims=True) + EPS)).astype(BF16)
                    return carry
                lax.fori_loop(0, batch // 32, body, 0)

            def forward(layer, h_in, h_out):
                rms_rows(h_in, layer)
                for blk in range(batch // ROW_BLOCK):
                    rows = pl.ds(blk * ROW_BLOCK, ROW_BLOCK)
                    slope[layer, rows] = jnp.dot(normed[layer, rows], wb1[layer], preferred_element_type=F32)

                    def gelu(i, carry):
                        at = pl.ds(pl.multiple_of(blk * ROW_BLOCK + i * 16, 16), 16)
                        for half in range(2):
                            lanes = pl.ds(half * (ff // 2), ff // 2)
                            z = slope[layer, at, lanes]
                            phi = 0.5 * (1.0 + lax.erf(z * INV_SQRT2))
                            act[layer, at, lanes] = (z * phi).astype(BF16)
                            slope[layer, at, lanes] = phi + z * jnp.exp(-0.5 * z * z) * INV_SQRT_2PI
                        return carry
                    lax.fori_loop(0, ROW_BLOCK // 16, gelu, 0)
                    h_out[rows] = (h_in[rows].astype(F32) + jnp.dot(act[layer, rows], wb2[layer], preferred_element_type=F32)).astype(BF16)

            forward(0, rows_buf.at[slot], hid.at[0])

            def forward_rest(layer, carry):
                forward(layer, hid.at[layer - 1], hid.at[layer])
                return carry
            lax.fori_loop(1, layers, forward_rest, 0)

            def loss(i, carry):
                at = pl.ds(pl.multiple_of(i * 32, 32), 32)
                e = (hid[layers - 1, at].astype(F32) - tgt_buf[slot, at].astype(F32)) * (2.0 / (batch * dim))
                grad_h[at] = e
                grad_bf[at] = e.astype(BF16)
                return carry
            lax.fori_loop(0, batch // 32, loss, 0)

            def apply(p, total, qb, layer, at, grad):
                if first:
                    total[layer, at] = grad
                    qb[layer, at] = (p[layer, at] - learn_rate * grad).astype(BF16)
                else:
                    total[layer, at] = learn_rate * (total[layer, at] + grad)

            def backward(back, carry):
                layer = layers - 1 - back
                for tile in range(ff // 256):
                    at = pl.ds(tile * 256, 256)
                    apply(p2, sum2, qb2, layer, at,
                          lax.dot_general(act[layer, :, at], grad_bf[...], CONTRACT_ROWS, preferred_element_type=F32))
                for blk in range(batch // ROW_BLOCK):
                    rows = pl.ds(blk * ROW_BLOCK, ROW_BLOCK)
                    d_pre[rows] = (lax.dot_general(grad_bf[rows], wb2[layer], CONTRACT_LAST, preferred_element_type=F32)
                                   * slope[layer, rows]).astype(BF16)
                for tile in range(dim // 128):
                    at = pl.ds(tile * 128, 128)
                    apply(p1, sum1, qb1, layer, at,
                          lax.dot_general(normed[layer, :, at], d_pre[...], CONTRACT_ROWS, preferred_element_type=F32))

                @pl.when(layer > 0)
                def _():
                    h_in = hid.at[layer - 1]
                    for blk in range(batch // ROW_BLOCK):
                        rows = pl.ds(blk * ROW_BLOCK, ROW_BLOCK)
                        grad_norm = lax.dot_general(d_pre[rows], wb1[layer], CONTRACT_LAST, preferred_element_type=F32)
                        h = h_in[rows].astype(F32)
                        inv_rms = lax.rsqrt(jnp.mean(h * h, axis=-1, keepdims=True) + EPS)
                        row_dot = jnp.mean(h * grad_norm, axis=-1, keepdims=True)
                        e = grad_h[rows] + (inv_rms * grad_norm - h * (inv_rms * inv_rms * inv_rms) * row_dot)
                        grad_h[rows] = e
                        grad_bf[rows] = e.astype(BF16)
                return carry
            lax.fori_loop(0, layers, backward, 0)

        def mix(window):
            slot = lax.rem(window, 2)

            def one(idx, carry):
                for which, (p, pb, total, got, stage) in enumerate(
                        ((p1, pb1, sum1, got1, stage1), (p2, pb2, sum2, got2, stage2))):
                    wait_all(sends(idx, slot, which))
                    layer, span = at_piece = piece(idx)[which]
                    staged = [pltpu.make_async_copy(got.at[(slot, k) + at_piece], stage.at[k], stage_sem.at[which, k])
                              for k in range(len(targets))]
                    start_all(staged)
                    wait_all(staged)
                    rows = stage.shape[1]
                    base = lax.rem(idx, PARTS) * rows

                    def some(i, inner):
                        src = pl.ds(pl.multiple_of(i * 16, 16), 16)
                        at = (layer, pl.ds(pl.multiple_of(base + i * 16, 16), 16))
                        acc = p[at] + stage[0, src].astype(F32)
                        acc = acc + stage[1, src].astype(F32)
                        other = stage[2, src].astype(F32)
                        acc = (acc + other) + other
                        new = acc / 5.0 - total[at]
                        p[at] = new
                        pb[at] = new.astype(BF16)
                        return inner
                    lax.fori_loop(0, rows // 16, some, 0)

                    @pl.when(window + 1 < windows)
                    def _():
                        start_all(sends(idx, 1 - slot, which))
                return carry
            lax.fori_loop(0, pieces, one, 0)

        def one_window(window, carry):
            local_step(2 * window, True, pb1, pb2)
            local_step(2 * window + 1, False, qb1, qb2)
            mix(window)
            return carry
        lax.fori_loop(0, windows, one_window, 0)

    def device_program(w_in, w_out, inputs, targets):
        layers, dim, ff = w_in.shape[2:]
        steps, batch = inputs.shape[2:4]
        pieces = layers * PARTS
        any_space = pl.BlockSpec(memory_space=pl.ANY)
        shape1, shape2 = (layers, dim, ff), (layers, ff, dim)
        sums = pl.pallas_call(
            device_kernel,
            out_shape=[pltpu.VMEM(shape1, F32), pltpu.VMEM(shape2, F32),
                       jax.ShapeDtypeStruct((2, 3) + shape1, BF16), jax.ShapeDtypeStruct((2, 3) + shape2, BF16)],
            in_specs=[any_space] * 4,
            out_specs=[pl.BlockSpec(memory_space=pltpu.VMEM)] * 2 + [any_space] * 2,
            scratch_shapes=[
                pltpu.VMEM(shape1, F32), pltpu.VMEM(shape2, F32),
                pltpu.VMEM(shape1, BF16), pltpu.VMEM(shape2, BF16),
                pltpu.VMEM(shape1, BF16), pltpu.VMEM(shape2, BF16),
                pltpu.VMEM((layers, batch, dim), BF16),
                pltpu.VMEM((layers, batch, dim), BF16),
                pltpu.VMEM((layers, batch, ff), F32),
                pltpu.VMEM((layers, batch, ff), BF16),
                pltpu.VMEM((batch, dim), F32),
                pltpu.VMEM((batch, dim), BF16),
                pltpu.VMEM((batch, ff), BF16),
                pltpu.VMEM((2, batch, dim), BF16), pltpu.VMEM((2, batch, dim), BF16),
                pltpu.VMEM((3, dim // PARTS, ff), BF16), pltpu.VMEM((3, ff // PARTS, dim), BF16),
                pltpu.SemaphoreType.DMA((pieces, 2)),
                pltpu.SemaphoreType.DMA((2, 2)),
                pltpu.SemaphoreType.DMA((2, 3)),
                pltpu.SemaphoreType.DMA((pieces, 2, 3)),
                pltpu.SemaphoreType.DMA((2, pieces, 2, 3)),
            ],
            compiler_params=pltpu.CompilerParams(collective_id=0, has_side_effects=True, vmem_limit_bytes=52_000_000),
        )(w_in[0, 0], w_out[0, 0], inputs[0, 0], targets[0, 0])
        return sums[0][None, None], sums[1][None, None]

    block_spec = P("row", "col")
    return jax.shard_map(device_program, mesh=mesh,
                         in_specs=(block_spec, block_spec, block_spec, block_spec),
                         out_specs=(block_spec, block_spec), check_vma=False)
```

```python
import jax
import jax.numpy as jnp
from jax import lax
from jax.experimental import pallas as pl
from jax.experimental.pallas import tpu as pltpu
from jax.sharding import PartitionSpec as P

LR_SCALE = 0.8
EPS = 1e-6
INV_SQRT2 = 0.7071067811865476
INV_SQRT_2PI = 0.3989422804014327
CONTRACT_ROWS = (((0,), (0,)), ((), ()))
CONTRACT_LAST = (((1,), (1,)), ((), ()))
MESH = pl.DeviceIdType.MESH
F32 = jnp.float32
BF16 = jnp.bfloat16

FIRST_ROWS = (64, 192)
LAST_ROWS = (256, 128)
ROW_BLOCK = 256


def exchange_table(layers, dim, ff):
    table, start = [], 0
    for part in FIRST_ROWS + (dim - sum(FIRST_ROWS),):
        table.append((0, 0, start, part))
        start += part
    table.append((1, 0, 0, ff))
    for layer in range(1, layers):
        table += [(0, layer, 0, dim), (1, layer, 0, ff)]
    which, layer, start, rows = table.pop()
    for part in (rows - sum(LAST_ROWS),) + LAST_ROWS:
        table.append((which, layer, start, part))
        start += part
    return table


def solution(mesh):
    col_size = mesh.shape["col"]

    def device_kernel(w1_hbm, w2_hbm, a_hbm, t_hbm, p1, p2, got1, got2,
                      sum1, sum2, pb1, pb2, qb1, qb2,
                      hid, normed, slope, act, grad_h, grad_bf, d_pre, rows_buf, tgt_buf, stage1, stage2, tail,
                      load_sem, data_sem, stage_sem, send_sem, recv_sem):
        layers, dim, ff = p1.shape
        batch = rows_buf.shape[1]
        steps = a_hbm.shape[0]
        windows = steps // 2
        learn_rate = LR_SCALE / layers
        params, bf_params, totals = (p1, p2), (pb1, pb2), (sum1, sum2)
        table = exchange_table(layers, dim, ff)

        row = lax.axis_index("row")
        col = lax.axis_index("col")
        targets = [(row, lax.rem(col + 1, col_size)), (row, lax.rem(col + col_size - 1, col_size)), (1 - row, col)]

        def span(idx):
            _, layer, start, rows = table[idx]
            return layer, pl.ds(start, rows)

        def landing(idx, slot, k):
            which, _, _, _ = table[idx]
            if idx == len(table) - 1:
                return tail.at[slot, k]
            return (got1, got2)[which].at[(slot, k) + span(idx)]

        def sends(idx, slot):
            src = bf_params[table[idx][0]].at[span(idx)]
            return [pltpu.make_async_remote_copy(
                src_ref=src, dst_ref=landing(idx, slot, k),
                send_sem=send_sem.at[idx, k], recv_sem=recv_sem.at[slot, idx, k],
                device_id=target, device_id_type=MESH) for k, target in enumerate(targets)]

        def load(idx):
            which = table[idx][0]
            return pltpu.make_async_copy((w1_hbm, w2_hbm)[which].at[span(idx)], params[which].at[span(idx)], load_sem.at[idx])

        def fetch(step):
            slot = lax.rem(step, 2)
            return [pltpu.make_async_copy(a_hbm.at[step], rows_buf.at[slot], data_sem.at[slot, 0]),
                    pltpu.make_async_copy(t_hbm.at[step], tgt_buf.at[slot], data_sem.at[slot, 1])]

        def start_all(copies):
            for copy in copies:
                copy.start()

        def wait_all(copies):
            for copy in copies:
                copy.wait()

        load(0).start()

        barrier = pltpu.get_barrier_semaphore()
        for target in targets:
            pl.semaphore_signal(barrier, inc=1, device_id=target, device_id_type=MESH)
        pl.semaphore_wait(barrier, len(targets))

        for idx, (which, layer, start, rows) in enumerate(table):
            if idx == 0:
                for later in range(1, len(table)):
                    load(later).start()
            load(idx).wait()
            p, pb = params[which], bf_params[which]

            def cast(i, carry):
                at = (layer, pl.ds(pl.multiple_of(start + i * 32, 32), 32))
                pb[at] = p[at].astype(BF16)
                return carry
            lax.fori_loop(0, rows // 32, cast, 0)
            start_all(sends(idx, 0))
        start_all(fetch(0))

        def local_step(step, first, wb1, wb2):
            slot = 0 if first else 1
            wait_all(fetch(step))
            @pl.when(step + 1 < steps)
            def _():
                start_all(fetch(step + 1))

            def rms_rows(src, layer):
                def body(i, carry):
                    at = pl.ds(pl.multiple_of(i * 32, 32), 32)
                    v = src[at].astype(F32)
                    normed[layer, at] = (v * lax.rsqrt(jnp.mean(v * v, axis=-1, keepdims=True) + EPS)).astype(BF16)
                    return carry
                lax.fori_loop(0, batch // 32, body, 0)

            def forward(layer, h_in, h_out):
                rms_rows(h_in, layer)
                for blk in range(batch // ROW_BLOCK):
                    rows = pl.ds(blk * ROW_BLOCK, ROW_BLOCK)
                    slope[layer, rows] = jnp.dot(normed[layer, rows], wb1[layer], preferred_element_type=F32)

                    def gelu(i, carry):
                        at = pl.ds(pl.multiple_of(blk * ROW_BLOCK + i * 16, 16), 16)
                        for half in range(2):
                            lanes = pl.ds(half * (ff // 2), ff // 2)
                            z = slope[layer, at, lanes]
                            phi = 0.5 * (1.0 + lax.erf(z * INV_SQRT2))
                            act[layer, at, lanes] = (z * phi).astype(BF16)
                            slope[layer, at, lanes] = phi + z * jnp.exp(-0.5 * z * z) * INV_SQRT_2PI
                        return carry
                    lax.fori_loop(0, ROW_BLOCK // 16, gelu, 0)
                    h_out[rows] = (h_in[rows].astype(F32) + jnp.dot(act[layer, rows], wb2[layer], preferred_element_type=F32)).astype(BF16)

            forward(0, rows_buf.at[slot], hid.at[0])

            def forward_rest(layer, carry):
                forward(layer, hid.at[layer - 1], hid.at[layer])
                return carry
            lax.fori_loop(1, layers, forward_rest, 0)

            def loss(i, carry):
                at = pl.ds(pl.multiple_of(i * 32, 32), 32)
                e = (hid[layers - 1, at].astype(F32) - tgt_buf[slot, at].astype(F32)) * (2.0 / (batch * dim))
                grad_h[at] = e
                grad_bf[at] = e.astype(BF16)
                return carry
            lax.fori_loop(0, batch // 32, loss, 0)

            def apply(p, total, qb, layer, at, grad):
                if first:
                    total[layer, at] = grad
                    qb[layer, at] = (p[layer, at] - learn_rate * grad).astype(BF16)
                else:
                    total[layer, at] = learn_rate * (total[layer, at] + grad)

            def backward(back, carry):
                layer = layers - 1 - back
                for tile in range(ff // 256):
                    at = pl.ds(tile * 256, 256)
                    apply(p2, sum2, qb2, layer, at,
                          lax.dot_general(act[layer, :, at], grad_bf[...], CONTRACT_ROWS, preferred_element_type=F32))
                for blk in range(batch // ROW_BLOCK):
                    rows = pl.ds(blk * ROW_BLOCK, ROW_BLOCK)
                    d_pre[rows] = (lax.dot_general(grad_bf[rows], wb2[layer], CONTRACT_LAST, preferred_element_type=F32)
                                   * slope[layer, rows]).astype(BF16)
                for tile in range(dim // 128):
                    at = pl.ds(tile * 128, 128)
                    apply(p1, sum1, qb1, layer, at,
                          lax.dot_general(normed[layer, :, at], d_pre[...], CONTRACT_ROWS, preferred_element_type=F32))

                @pl.when(layer > 0)
                def _():
                    h_in = hid.at[layer - 1]
                    for blk in range(batch // ROW_BLOCK):
                        rows = pl.ds(blk * ROW_BLOCK, ROW_BLOCK)
                        grad_norm = lax.dot_general(d_pre[rows], wb1[layer], CONTRACT_LAST, preferred_element_type=F32)
                        h = h_in[rows].astype(F32)
                        inv_rms = lax.rsqrt(jnp.mean(h * h, axis=-1, keepdims=True) + EPS)
                        row_dot = jnp.mean(h * grad_norm, axis=-1, keepdims=True)
                        e = grad_h[rows] + (inv_rms * grad_norm - h * (inv_rms * inv_rms * inv_rms) * row_dot)
                        grad_h[rows] = e
                        grad_bf[rows] = e.astype(BF16)
                return carry
            lax.fori_loop(0, layers, backward, 0)

        def mix(window):
            slot = lax.rem(window, 2)

            for idx, (which, layer, start, rows) in enumerate(table):
                p, pb, total = params[which], bf_params[which], totals[which]
                wait_all(sends(idx, slot))
                if idx == len(table) - 1:
                    stage = tail.at[slot]
                else:
                    stage = (stage1, stage2)[which]
                    staged = [pltpu.make_async_copy(landing(idx, slot, k), stage.at[k, pl.ds(0, rows)], stage_sem.at[which, k])
                              for k in range(len(targets))]
                    start_all(staged)
                    wait_all(staged)

                def some(i, carry):
                    src = pl.ds(pl.multiple_of(i * 16, 16), 16)
                    at = (layer, pl.ds(pl.multiple_of(start + i * 16, 16), 16))
                    acc = p[at] + stage[0, src].astype(F32)
                    acc = acc + stage[1, src].astype(F32)
                    other = stage[2, src].astype(F32)
                    acc = (acc + other) + other
                    new = acc / 5.0 - total[at]
                    p[at] = new
                    pb[at] = new.astype(BF16)
                    return carry
                lax.fori_loop(0, rows // 16, some, 0)

                @pl.when(window + 1 < windows)
                def _():
                    start_all(sends(idx, 1 - slot))

        def one_window(window, carry):
            local_step(2 * window, True, pb1, pb2)
            local_step(2 * window + 1, False, qb1, qb2)
            mix(window)
            return carry
        lax.fori_loop(0, windows, one_window, 0)

    def device_program(w_in, w_out, inputs, targets):
        layers, dim, ff = w_in.shape[2:]
        steps, batch = inputs.shape[2:4]
        pieces = len(exchange_table(layers, dim, ff))
        any_space = pl.BlockSpec(memory_space=pl.ANY)
        shape1, shape2 = (layers, dim, ff), (layers, ff, dim)
        sums = pl.pallas_call(
            device_kernel,
            out_shape=[pltpu.VMEM(shape1, F32), pltpu.VMEM(shape2, F32),
                       jax.ShapeDtypeStruct((2, 3) + shape1, BF16), jax.ShapeDtypeStruct((2, 3) + shape2, BF16)],
            in_specs=[any_space] * 4,
            out_specs=[pl.BlockSpec(memory_space=pltpu.VMEM)] * 2 + [any_space] * 2,
            scratch_shapes=[
                pltpu.VMEM(shape1, F32), pltpu.VMEM(shape2, F32),
                pltpu.VMEM(shape1, BF16), pltpu.VMEM(shape2, BF16),
                pltpu.VMEM(shape1, BF16), pltpu.VMEM(shape2, BF16),
                pltpu.VMEM((layers, batch, dim), BF16),
                pltpu.VMEM((layers, batch, dim), BF16),
                pltpu.VMEM((layers, batch, ff), F32),
                pltpu.VMEM((layers, batch, ff), BF16),
                pltpu.VMEM((batch, dim), F32),
                pltpu.VMEM((batch, dim), BF16),
                pltpu.VMEM((batch, ff), BF16),
                pltpu.VMEM((2, batch, dim), BF16), pltpu.VMEM((2, batch, dim), BF16),
                pltpu.VMEM((3, dim, ff), BF16), pltpu.VMEM((3, ff, dim), BF16),
                pltpu.VMEM((2, 3, LAST_ROWS[-1], dim), BF16),
                pltpu.SemaphoreType.DMA((pieces,)),
                pltpu.SemaphoreType.DMA((2, 2)),
                pltpu.SemaphoreType.DMA((2, 3)),
                pltpu.SemaphoreType.DMA((pieces, 3)),
                pltpu.SemaphoreType.DMA((2, pieces, 3)),
            ],
            compiler_params=pltpu.CompilerParams(collective_id=0, has_side_effects=True, vmem_limit_bytes=52_000_000),
        )(w_in[0, 0], w_out[0, 0], inputs[0, 0], targets[0, 0])

        def store_kernel(p1, p2, out1, out2, sem):
            copies = []
            for idx in range(layers):
                copies.append(pltpu.make_async_copy(p1.at[idx], out1.at[idx], sem.at[0, idx]))
                copies.append(pltpu.make_async_copy(p2.at[idx], out2.at[idx], sem.at[1, idx]))
            for copy in copies:
                copy.start()
            for copy in copies:
                copy.wait()

        new_in, new_out = pl.pallas_call(
            store_kernel,
            out_shape=[jax.ShapeDtypeStruct(shape1, F32), jax.ShapeDtypeStruct(shape2, F32)],
            in_specs=[pl.BlockSpec(memory_space=pltpu.VMEM)] * 2,
            out_specs=[any_space] * 2,
            scratch_shapes=[pltpu.SemaphoreType.DMA((2, layers))],
            compiler_params=pltpu.CompilerParams(vmem_limit_bytes=30_000_000),
        )(sums[0], sums[1])
        return new_in[None, None], new_out[None, None]

    block_spec = P("row", "col")
    return jax.shard_map(device_program, mesh=mesh,
                         in_specs=(block_spec, block_spec, block_spec, block_spec),
                         out_specs=(block_spec, block_spec), check_vma=False)
```

```python
import jax
import jax.numpy as jnp
from jax import lax
from jax.experimental import pallas as pl
from jax.experimental.pallas import tpu as pltpu
from jax.sharding import PartitionSpec as P

LR_SCALE = 0.8
EPS = 1e-6
INV_SQRT2 = 0.7071067811865476
INV_SQRT_2PI = 0.3989422804014327
CONTRACT_ROWS = (((0,), (0,)), ((), ()))
CONTRACT_LAST = (((1,), (1,)), ((), ()))
MESH = pl.DeviceIdType.MESH
F32 = jnp.float32
BF16 = jnp.bfloat16

FIRST_ROWS = (64,)
LAST_ROWS = (256,)
ROW_BLOCK = 256


def exchange_table(layers, dim, ff):
    table, start = [], 0
    for part in FIRST_ROWS + (dim - sum(FIRST_ROWS),):
        table.append((0, 0, start, part))
        start += part
    table.append((1, 0, 0, ff))
    for layer in range(1, layers):
        table += [(0, layer, 0, dim), (1, layer, 0, ff)]
    which, layer, start, rows = table.pop()
    for part in (rows - sum(LAST_ROWS),) + LAST_ROWS:
        table.append((which, layer, start, part))
        start += part
    return table


def solution(mesh):
    col_size = mesh.shape["col"]

    def device_kernel(w1_hbm, w2_hbm, a_hbm, t_hbm, p1, p2, got1, got2, tail, tail_total,
                      sum1, sum2, pb1, pb2, qb1, qb2,
                      hid, normed, slope, act, grad_h, grad_bf, d_pre, rows_buf, tgt_buf, stage1, stage2,
                      load_sem, data_sem, stage_sem, send_sem, recv_sem):
        layers, dim, ff = p1.shape
        batch = rows_buf.shape[1]
        steps = a_hbm.shape[0]
        windows = steps // 2
        learn_rate = LR_SCALE / layers
        params, bf_params, totals = (p1, p2), (pb1, pb2), (sum1, sum2)
        table = exchange_table(layers, dim, ff)

        row = lax.axis_index("row")
        col = lax.axis_index("col")
        targets = [(row, lax.rem(col + 1, col_size)), (row, lax.rem(col + col_size - 1, col_size)), (1 - row, col)]

        def span(idx):
            _, layer, start, rows = table[idx]
            return layer, pl.ds(start, rows)

        def landing(idx, slot, k):
            which, _, _, _ = table[idx]
            if idx == len(table) - 1:
                return tail.at[slot, k]
            return (got1, got2)[which].at[(slot, k) + span(idx)]

        def sends(idx, slot):
            src = bf_params[table[idx][0]].at[span(idx)]
            return [pltpu.make_async_remote_copy(
                src_ref=src, dst_ref=landing(idx, slot, k),
                send_sem=send_sem.at[idx, k], recv_sem=recv_sem.at[slot, idx, k],
                device_id=target, device_id_type=MESH) for k, target in enumerate(targets)]

        def load(idx):
            which = table[idx][0]
            return pltpu.make_async_copy((w1_hbm, w2_hbm)[which].at[span(idx)], params[which].at[span(idx)], load_sem.at[idx])

        def fetch(step):
            slot = lax.rem(step, 2)
            return [pltpu.make_async_copy(a_hbm.at[step], rows_buf.at[slot], data_sem.at[slot, 0]),
                    pltpu.make_async_copy(t_hbm.at[step], tgt_buf.at[slot], data_sem.at[slot, 1])]

        def start_all(copies):
            for copy in copies:
                copy.start()

        def wait_all(copies):
            for copy in copies:
                copy.wait()

        load(0).start()

        barrier = pltpu.get_barrier_semaphore()
        for target in targets:
            pl.semaphore_signal(barrier, inc=1, device_id=target, device_id_type=MESH)
        pl.semaphore_wait(barrier, len(targets))

        for idx, (which, layer, start, rows) in enumerate(table):
            if idx == 0:
                for later in range(1, len(table)):
                    load(later).start()
            load(idx).wait()
            p, pb = params[which], bf_params[which]

            def cast(i, carry):
                at = (layer, pl.ds(pl.multiple_of(start + i * 32, 32), 32))
                pb[at] = p[at].astype(BF16)
                return carry
            lax.fori_loop(0, rows // 32, cast, 0)
            start_all(sends(idx, 0))
        start_all(fetch(0))

        def local_step(step, first, wb1, wb2):
            slot = 0 if first else 1
            wait_all(fetch(step))
            @pl.when(step + 1 < steps)
            def _():
                start_all(fetch(step + 1))

            def rms_rows(src, layer):
                def body(i, carry):
                    at = pl.ds(pl.multiple_of(i * 32, 32), 32)
                    v = src[at].astype(F32)
                    normed[layer, at] = (v * lax.rsqrt(jnp.mean(v * v, axis=-1, keepdims=True) + EPS)).astype(BF16)
                    return carry
                lax.fori_loop(0, batch // 32, body, 0)

            def forward(layer, h_in, h_out):
                rms_rows(h_in, layer)
                for blk in range(batch // ROW_BLOCK):
                    rows = pl.ds(blk * ROW_BLOCK, ROW_BLOCK)
                    slope[layer, rows] = jnp.dot(normed[layer, rows], wb1[layer], preferred_element_type=F32)

                    def gelu(i, carry):
                        at = pl.ds(pl.multiple_of(blk * ROW_BLOCK + i * 16, 16), 16)
                        for half in range(2):
                            lanes = pl.ds(half * (ff // 2), ff // 2)
                            z = slope[layer, at, lanes]
                            phi = 0.5 * (1.0 + lax.erf(z * INV_SQRT2))
                            act[layer, at, lanes] = (z * phi).astype(BF16)
                            slope[layer, at, lanes] = phi + z * jnp.exp(-0.5 * z * z) * INV_SQRT_2PI
                        return carry
                    lax.fori_loop(0, ROW_BLOCK // 16, gelu, 0)
                    h_out[rows] = (h_in[rows].astype(F32) + jnp.dot(act[layer, rows], wb2[layer], preferred_element_type=F32)).astype(BF16)

            forward(0, rows_buf.at[slot], hid.at[0])

            def forward_rest(layer, carry):
                forward(layer, hid.at[layer - 1], hid.at[layer])
                return carry
            lax.fori_loop(1, layers, forward_rest, 0)

            def loss(i, carry):
                at = pl.ds(pl.multiple_of(i * 32, 32), 32)
                e = (hid[layers - 1, at].astype(F32) - tgt_buf[slot, at].astype(F32)) * (2.0 / (batch * dim))
                grad_h[at] = e
                grad_bf[at] = e.astype(BF16)
                return carry
            lax.fori_loop(0, batch // 32, loss, 0)

            def apply(p, total, qb, layer, at, grad):
                if first:
                    total[layer, at] = grad
                    qb[layer, at] = (p[layer, at] - learn_rate * grad).astype(BF16)
                else:
                    total[layer, at] = learn_rate * (total[layer, at] + grad)

            def backward(back, carry):
                layer = layers - 1 - back
                for tile in range(ff // 256):
                    at = pl.ds(tile * 256, 256)
                    apply(p2, sum2, qb2, layer, at,
                          lax.dot_general(act[layer, :, at], grad_bf[...], CONTRACT_ROWS, preferred_element_type=F32))
                for blk in range(batch // ROW_BLOCK):
                    rows = pl.ds(blk * ROW_BLOCK, ROW_BLOCK)
                    d_pre[rows] = (lax.dot_general(grad_bf[rows], wb2[layer], CONTRACT_LAST, preferred_element_type=F32)
                                   * slope[layer, rows]).astype(BF16)
                for tile in range(dim // 128):
                    at = pl.ds(tile * 128, 128)
                    apply(p1, sum1, qb1, layer, at,
                          lax.dot_general(normed[layer, :, at], d_pre[...], CONTRACT_ROWS, preferred_element_type=F32))

                @pl.when(layer > 0)
                def _():
                    h_in = hid.at[layer - 1]
                    for blk in range(batch // ROW_BLOCK):
                        rows = pl.ds(blk * ROW_BLOCK, ROW_BLOCK)
                        grad_norm = lax.dot_general(d_pre[rows], wb1[layer], CONTRACT_LAST, preferred_element_type=F32)
                        h = h_in[rows].astype(F32)
                        inv_rms = lax.rsqrt(jnp.mean(h * h, axis=-1, keepdims=True) + EPS)
                        row_dot = jnp.mean(h * grad_norm, axis=-1, keepdims=True)
                        e = grad_h[rows] + (inv_rms * grad_norm - h * (inv_rms * inv_rms * inv_rms) * row_dot)
                        grad_h[rows] = e
                        grad_bf[rows] = e.astype(BF16)
                return carry
            lax.fori_loop(0, layers, backward, 0)

        def mix(window):
            slot = lax.rem(window, 2)

            for idx, (which, layer, start, rows) in enumerate(table):
                p, pb, total = params[which], bf_params[which], totals[which]
                if idx == len(table) - 1:
                    def keep(i, carry):
                        at = pl.ds(pl.multiple_of(i * 32, 32), 32)
                        tail_total[at] = total[layer, pl.ds(pl.multiple_of(start + i * 32, 32), 32)]
                        return carry
                    lax.fori_loop(0, rows // 32, keep, 0)
                wait_all(sends(idx, slot))
                if idx == len(table) - 1:
                    stage = tail.at[slot]
                else:
                    stage = (stage1, stage2)[which]
                    staged = [pltpu.make_async_copy(landing(idx, slot, k), stage.at[k, pl.ds(0, rows)], stage_sem.at[which, k])
                              for k in range(len(targets))]
                    start_all(staged)
                    wait_all(staged)

                def some(i, carry):
                    src = pl.ds(pl.multiple_of(i * 16, 16), 16)
                    at = (layer, pl.ds(pl.multiple_of(start + i * 16, 16), 16))
                    acc = p[at] + stage[0, src].astype(F32)
                    acc = acc + stage[1, src].astype(F32)
                    other = stage[2, src].astype(F32)
                    acc = (acc + other) + other
                    new = acc / 5.0 - total[at]
                    p[at] = new
                    pb[at] = new.astype(BF16)
                    return carry
                if idx < len(table) - 1:
                    lax.fori_loop(0, rows // 16, some, 0)

                @pl.when(window + 1 < windows)
                def _():
                    if idx == len(table) - 1:
                        lax.fori_loop(0, rows // 16, some, 0)
                    start_all(sends(idx, 1 - slot))

        def one_window(window, carry):
            local_step(2 * window, True, pb1, pb2)
            local_step(2 * window + 1, False, qb1, qb2)
            mix(window)
            return carry
        lax.fori_loop(0, windows, one_window, 0)

    def device_program(w_in, w_out, inputs, targets):
        layers, dim, ff = w_in.shape[2:]
        steps, batch = inputs.shape[2:4]
        pieces = len(exchange_table(layers, dim, ff))
        any_space = pl.BlockSpec(memory_space=pl.ANY)
        shape1, shape2 = (layers, dim, ff), (layers, ff, dim)
        sums = pl.pallas_call(
            device_kernel,
            out_shape=[pltpu.VMEM(shape1, F32), pltpu.VMEM(shape2, F32),
                       jax.ShapeDtypeStruct((2, 3) + shape1, BF16), jax.ShapeDtypeStruct((2, 3) + shape2, BF16),
                       pltpu.VMEM((2, 3, LAST_ROWS[-1], dim), BF16), pltpu.VMEM((LAST_ROWS[-1], dim), F32)],
            in_specs=[any_space] * 4,
            out_specs=([pl.BlockSpec(memory_space=pltpu.VMEM)] * 2 + [any_space] * 2
                       + [pl.BlockSpec(memory_space=pltpu.VMEM)] * 2),
            scratch_shapes=[
                pltpu.VMEM(shape1, F32), pltpu.VMEM(shape2, F32),
                pltpu.VMEM(shape1, BF16), pltpu.VMEM(shape2, BF16),
                pltpu.VMEM(shape1, BF16), pltpu.VMEM(shape2, BF16),
                pltpu.VMEM((layers, batch, dim), BF16),
                pltpu.VMEM((layers, batch, dim), BF16),
                pltpu.VMEM((layers, batch, ff), F32),
                pltpu.VMEM((layers, batch, ff), BF16),
                pltpu.VMEM((batch, dim), F32),
                pltpu.VMEM((batch, dim), BF16),
                pltpu.VMEM((batch, ff), BF16),
                pltpu.VMEM((2, batch, dim), BF16), pltpu.VMEM((2, batch, dim), BF16),
                pltpu.VMEM((3, dim, ff), BF16), pltpu.VMEM((3, ff, dim), BF16),
                pltpu.SemaphoreType.DMA((pieces,)),
                pltpu.SemaphoreType.DMA((2, 2)),
                pltpu.SemaphoreType.DMA((2, 3)),
                pltpu.SemaphoreType.DMA((pieces, 3)),
                pltpu.SemaphoreType.DMA((2, pieces, 3)),
            ],
            compiler_params=pltpu.CompilerParams(collective_id=0, has_side_effects=True, vmem_limit_bytes=52_000_000),
        )(w_in[0, 0], w_out[0, 0], inputs[0, 0], targets[0, 0])

        last_slot = (steps // 2 - 1) % 2

        def store_kernel(p1, p2, tail, tail_total, out1, out2, last, sem):
            rows = tail_total.shape[0]
            copies = []
            for idx in range(layers):
                copies.append(pltpu.make_async_copy(p1.at[idx], out1.at[idx], sem.at[0, idx]))
                at = (idx, pl.ds(0, ff - rows if idx == layers - 1 else ff))
                copies.append(pltpu.make_async_copy(p2.at[at], out2.at[at], sem.at[1, idx]))
            for copy in copies:
                copy.start()

            def some(i, carry):
                src = pl.ds(pl.multiple_of(i * 16, 16), 16)
                acc = p2[layers - 1, pl.ds(pl.multiple_of(ff - rows + i * 16, 16), 16)] + tail[last_slot, 0, src].astype(F32)
                acc = acc + tail[last_slot, 1, src].astype(F32)
                other = tail[last_slot, 2, src].astype(F32)
                last[src] = ((acc + other) + other) / 5.0 - tail_total[src]
                return carry
            lax.fori_loop(0, rows // 16, some, 0)
            copies.append(pltpu.make_async_copy(last, out2.at[layers - 1, pl.ds(ff - rows, rows)], sem.at[0, layers]))
            copies[-1].start()
            for copy in copies:
                copy.wait()

        new_in, new_out = pl.pallas_call(
            store_kernel,
            out_shape=[jax.ShapeDtypeStruct(shape1, F32), jax.ShapeDtypeStruct(shape2, F32)],
            in_specs=[pl.BlockSpec(memory_space=pltpu.VMEM)] * 4,
            out_specs=[any_space] * 2,
            scratch_shapes=[pltpu.VMEM((LAST_ROWS[-1], dim), F32), pltpu.SemaphoreType.DMA((2, layers + 1))],
            compiler_params=pltpu.CompilerParams(vmem_limit_bytes=30_000_000),
        )(sums[0], sums[1], sums[4], sums[5])
        return new_in[None, None], new_out[None, None]

    block_spec = P("row", "col")
    return jax.shard_map(device_program, mesh=mesh,
                         in_specs=(block_spec, block_spec, block_spec, block_spec),
                         out_specs=(block_spec, block_spec), check_vma=False)
```

```python
import jax
import jax.numpy as jnp
from jax import lax
from jax.experimental import pallas as pl
from jax.experimental.pallas import tpu as pltpu
from jax.sharding import PartitionSpec as P

LR_SCALE = 0.8
EPS = 1e-6
INV_SQRT2 = 0.7071067811865476
INV_SQRT_2PI = 0.3989422804014327
CONTRACT_ROWS = (((0,), (0,)), ((), ()))
CONTRACT_LAST = (((1,), (1,)), ((), ()))
MESH = pl.DeviceIdType.MESH
F32 = jnp.float32
BF16 = jnp.bfloat16

FIRST_ROWS = (64,)
LAST_ROWS = (256,)
ROW_BLOCK = 256


def exchange_table(layers, dim, ff):
    table, start = [], 0
    for part in FIRST_ROWS + (dim - sum(FIRST_ROWS),):
        table.append((0, 0, start, part))
        start += part
    table.append((1, 0, 0, ff))
    for layer in range(1, layers):
        table += [(0, layer, 0, dim), (1, layer, 0, ff)]
    which, layer, start, rows = table.pop()
    for part in (rows - sum(LAST_ROWS),) + LAST_ROWS:
        table.append((which, layer, start, part))
        start += part
    return table


def solution(mesh):
    col_size = mesh.shape["col"]

    def device_kernel(w1_hbm, w2_hbm, a_hbm, t_hbm, p1, p2, got1, got2, tail, tail_total,
                      sum1, sum2, pb1, pb2, qb1, qb2,
                      hid, normed, slope, act, grad_h, grad_bf, d_pre, rows_buf, tgt_buf, stage1, stage2,
                      load_sem, data_sem, stage_sem, send_sem, recv_sem):
        layers, dim, ff = p1.shape
        batch = rows_buf.shape[1]
        steps = a_hbm.shape[0]
        windows = steps // 2
        learn_rate = LR_SCALE / layers
        params, bf_params, totals = (p1, p2), (pb1, pb2), (sum1, sum2)
        table = exchange_table(layers, dim, ff)

        row = lax.axis_index("row")
        col = lax.axis_index("col")
        targets = [(row, lax.rem(col + 1, col_size)), (row, lax.rem(col + col_size - 1, col_size)), (1 - row, col)]

        def span(idx):
            _, layer, start, rows = table[idx]
            return layer, pl.ds(start, rows)

        def landing(idx, slot, k):
            which, _, _, _ = table[idx]
            if idx == len(table) - 1:
                return tail.at[slot, k]
            return (got1, got2)[which].at[(slot, k) + span(idx)]

        def sends(idx, slot):
            src = bf_params[table[idx][0]].at[span(idx)]
            return [pltpu.make_async_remote_copy(
                src_ref=src, dst_ref=landing(idx, slot, k),
                send_sem=send_sem.at[idx, k], recv_sem=recv_sem.at[slot, idx, k],
                device_id=target, device_id_type=MESH) for k, target in enumerate(targets)]

        def load(idx):
            which = table[idx][0]
            return pltpu.make_async_copy((w1_hbm, w2_hbm)[which].at[span(idx)], params[which].at[span(idx)], load_sem.at[idx])

        def fetch(step):
            slot = lax.rem(step, 2)
            return [pltpu.make_async_copy(a_hbm.at[step], rows_buf.at[slot], data_sem.at[slot, 0]),
                    pltpu.make_async_copy(t_hbm.at[step], tgt_buf.at[slot], data_sem.at[slot, 1])]

        def start_all(copies):
            for copy in reversed(copies):
                copy.start()

        def wait_all(copies):
            for copy in copies:
                copy.wait()

        load(0).start()

        barrier = pltpu.get_barrier_semaphore()
        for target in targets:
            pl.semaphore_signal(barrier, inc=1, device_id=target, device_id_type=MESH)
        pl.semaphore_wait(barrier, len(targets))

        for idx, (which, layer, start, rows) in enumerate(table):
            if idx == 0:
                for later in range(1, len(table)):
                    load(later).start()
            load(idx).wait()
            p, pb = params[which], bf_params[which]

            def cast(i, carry):
                at = (layer, pl.ds(pl.multiple_of(start + i * 32, 32), 32))
                pb[at] = p[at].astype(BF16)
                return carry
            lax.fori_loop(0, rows // 32, cast, 0)
            start_all(sends(idx, 0))
        start_all(fetch(0))

        def local_step(step, first, wb1, wb2):
            slot = 0 if first else 1
            wait_all(fetch(step))
            @pl.when(step + 1 < steps)
            def _():
                start_all(fetch(step + 1))

            def rms_rows(src, layer):
                def body(i, carry):
                    at = pl.ds(pl.multiple_of(i * 32, 32), 32)
                    v = src[at].astype(F32)
                    normed[layer, at] = (v * lax.rsqrt(jnp.mean(v * v, axis=-1, keepdims=True) + EPS)).astype(BF16)
                    return carry
                lax.fori_loop(0, batch // 32, body, 0)

            def forward(layer, h_in, h_out):
                rms_rows(h_in, layer)
                for blk in range(batch // ROW_BLOCK):
                    rows = pl.ds(blk * ROW_BLOCK, ROW_BLOCK)
                    slope[layer, rows] = jnp.dot(normed[layer, rows], wb1[layer], preferred_element_type=F32)

                    def gelu(i, carry):
                        at = pl.ds(pl.multiple_of(blk * ROW_BLOCK + i * 16, 16), 16)
                        for half in range(2):
                            lanes = pl.ds(half * (ff // 2), ff // 2)
                            z = slope[layer, at, lanes]
                            phi = 0.5 * (1.0 + lax.erf(z * INV_SQRT2))
                            act[layer, at, lanes] = (z * phi).astype(BF16)
                            slope[layer, at, lanes] = phi + z * jnp.exp(-0.5 * z * z) * INV_SQRT_2PI
                        return carry
                    lax.fori_loop(0, ROW_BLOCK // 16, gelu, 0)
                    h_out[rows] = (h_in[rows].astype(F32) + jnp.dot(act[layer, rows], wb2[layer], preferred_element_type=F32)).astype(BF16)

            forward(0, rows_buf.at[slot], hid.at[0])

            def forward_rest(layer, carry):
                forward(layer, hid.at[layer - 1], hid.at[layer])
                return carry
            lax.fori_loop(1, layers, forward_rest, 0)

            def loss(i, carry):
                at = pl.ds(pl.multiple_of(i * 32, 32), 32)
                e = (hid[layers - 1, at].astype(F32) - tgt_buf[slot, at].astype(F32)) * (2.0 / (batch * dim))
                grad_h[at] = e
                grad_bf[at] = e.astype(BF16)
                return carry
            lax.fori_loop(0, batch // 32, loss, 0)

            def apply(p, total, qb, layer, at, grad):
                if first:
                    total[layer, at] = grad
                    qb[layer, at] = (p[layer, at] - learn_rate * grad).astype(BF16)
                else:
                    total[layer, at] = learn_rate * (total[layer, at] + grad)

            def backward(back, carry):
                layer = layers - 1 - back
                for tile in range(ff // 256):
                    at = pl.ds(tile * 256, 256)
                    apply(p2, sum2, qb2, layer, at,
                          lax.dot_general(act[layer, :, at], grad_bf[...], CONTRACT_ROWS, preferred_element_type=F32))
                for blk in range(batch // ROW_BLOCK):
                    rows = pl.ds(blk * ROW_BLOCK, ROW_BLOCK)
                    d_pre[rows] = (lax.dot_general(grad_bf[rows], wb2[layer], CONTRACT_LAST, preferred_element_type=F32)
                                   * slope[layer, rows]).astype(BF16)
                for tile in range(dim // 128):
                    at = pl.ds(tile * 128, 128)
                    apply(p1, sum1, qb1, layer, at,
                          lax.dot_general(normed[layer, :, at], d_pre[...], CONTRACT_ROWS, preferred_element_type=F32))

                @pl.when(layer > 0)
                def _():
                    h_in = hid.at[layer - 1]
                    for blk in range(batch // ROW_BLOCK):
                        rows = pl.ds(blk * ROW_BLOCK, ROW_BLOCK)
                        grad_norm = lax.dot_general(d_pre[rows], wb1[layer], CONTRACT_LAST, preferred_element_type=F32)
                        h = h_in[rows].astype(F32)
                        inv_rms = lax.rsqrt(jnp.mean(h * h, axis=-1, keepdims=True) + EPS)
                        row_dot = jnp.mean(h * grad_norm, axis=-1, keepdims=True)
                        e = grad_h[rows] + (inv_rms * grad_norm - h * (inv_rms * inv_rms * inv_rms) * row_dot)
                        grad_h[rows] = e
                        grad_bf[rows] = e.astype(BF16)
                return carry
            lax.fori_loop(0, layers, backward, 0)

        def mix(window):
            slot = lax.rem(window, 2)

            for idx, (which, layer, start, rows) in enumerate(table):
                p, pb, total = params[which], bf_params[which], totals[which]
                if idx == len(table) - 1:
                    def keep(i, carry):
                        at = pl.ds(pl.multiple_of(i * 32, 32), 32)
                        tail_total[at] = total[layer, pl.ds(pl.multiple_of(start + i * 32, 32), 32)]
                        return carry
                    lax.fori_loop(0, rows // 32, keep, 0)
                wait_all(sends(idx, slot))
                if idx == len(table) - 1:
                    stage = tail.at[slot]
                else:
                    stage = (stage1, stage2)[which]
                    staged = [pltpu.make_async_copy(landing(idx, slot, k), stage.at[k, pl.ds(0, rows)], stage_sem.at[which, k])
                              for k in range(len(targets))]
                    start_all(staged)
                    wait_all(staged)

                def some(i, carry):
                    src = pl.ds(pl.multiple_of(i * 16, 16), 16)
                    at = (layer, pl.ds(pl.multiple_of(start + i * 16, 16), 16))
                    acc = p[at] + stage[0, src].astype(F32)
                    acc = acc + stage[1, src].astype(F32)
                    other = stage[2, src].astype(F32)
                    acc = (acc + other) + other
                    new = acc / 5.0 - total[at]
                    p[at] = new
                    pb[at] = new.astype(BF16)
                    return carry
                if idx < len(table) - 1:
                    lax.fori_loop(0, rows // 16, some, 0)

                @pl.when(window + 1 < windows)
                def _():
                    if idx == len(table) - 1:
                        lax.fori_loop(0, rows // 16, some, 0)
                    start_all(sends(idx, 1 - slot))

        def one_window(window, carry):
            local_step(2 * window, True, pb1, pb2)
            local_step(2 * window + 1, False, qb1, qb2)
            mix(window)
            return carry
        lax.fori_loop(0, windows, one_window, 0)

    def device_program(w_in, w_out, inputs, targets):
        layers, dim, ff = w_in.shape[2:]
        steps, batch = inputs.shape[2:4]
        pieces = len(exchange_table(layers, dim, ff))
        any_space = pl.BlockSpec(memory_space=pl.ANY)
        shape1, shape2 = (layers, dim, ff), (layers, ff, dim)
        sums = pl.pallas_call(
            device_kernel,
            out_shape=[pltpu.VMEM(shape1, F32), pltpu.VMEM(shape2, F32),
                       jax.ShapeDtypeStruct((2, 3) + shape1, BF16), jax.ShapeDtypeStruct((2, 3) + shape2, BF16),
                       pltpu.VMEM((2, 3, LAST_ROWS[-1], dim), BF16), pltpu.VMEM((LAST_ROWS[-1], dim), F32)],
            in_specs=[any_space] * 4,
            out_specs=([pl.BlockSpec(memory_space=pltpu.VMEM)] * 2 + [any_space] * 2
                       + [pl.BlockSpec(memory_space=pltpu.VMEM)] * 2),
            scratch_shapes=[
                pltpu.VMEM(shape1, F32), pltpu.VMEM(shape2, F32),
                pltpu.VMEM(shape1, BF16), pltpu.VMEM(shape2, BF16),
                pltpu.VMEM(shape1, BF16), pltpu.VMEM(shape2, BF16),
                pltpu.VMEM((layers, batch, dim), BF16),
                pltpu.VMEM((layers, batch, dim), BF16),
                pltpu.VMEM((layers, batch, ff), F32),
                pltpu.VMEM((layers, batch, ff), BF16),
                pltpu.VMEM((batch, dim), F32),
                pltpu.VMEM((batch, dim), BF16),
                pltpu.VMEM((batch, ff), BF16),
                pltpu.VMEM((2, batch, dim), BF16), pltpu.VMEM((2, batch, dim), BF16),
                pltpu.VMEM((3, dim, ff), BF16), pltpu.VMEM((3, ff, dim), BF16),
                pltpu.SemaphoreType.DMA((pieces,)),
                pltpu.SemaphoreType.DMA((2, 2)),
                pltpu.SemaphoreType.DMA((2, 3)),
                pltpu.SemaphoreType.DMA((pieces, 3)),
                pltpu.SemaphoreType.DMA((2, pieces, 3)),
            ],
            compiler_params=pltpu.CompilerParams(collective_id=0, has_side_effects=True, vmem_limit_bytes=52_000_000),
        )(w_in[0, 0], w_out[0, 0], inputs[0, 0], targets[0, 0])

        last_slot = (steps // 2 - 1) % 2

        def store_kernel(p1, p2, tail, tail_total, out1, out2, last, sem):
            rows = tail_total.shape[0]
            copies = []
            for idx in range(layers):
                copies.append(pltpu.make_async_copy(p1.at[idx], out1.at[idx], sem.at[0, idx]))
                at = (idx, pl.ds(0, ff - rows if idx == layers - 1 else ff))
                copies.append(pltpu.make_async_copy(p2.at[at], out2.at[at], sem.at[1, idx]))
            for copy in copies:
                copy.start()

            def some(i, carry):
                src = pl.ds(pl.multiple_of(i * 16, 16), 16)
                acc = p2[layers - 1, pl.ds(pl.multiple_of(ff - rows + i * 16, 16), 16)] + tail[last_slot, 0, src].astype(F32)
                acc = acc + tail[last_slot, 1, src].astype(F32)
                other = tail[last_slot, 2, src].astype(F32)
                last[src] = ((acc + other) + other) / 5.0 - tail_total[src]
                return carry
            lax.fori_loop(0, rows // 16, some, 0)
            copies.append(pltpu.make_async_copy(last, out2.at[layers - 1, pl.ds(ff - rows, rows)], sem.at[0, layers]))
            copies[-1].start()
            for copy in copies:
                copy.wait()

        new_in, new_out = pl.pallas_call(
            store_kernel,
            out_shape=[jax.ShapeDtypeStruct(shape1, F32), jax.ShapeDtypeStruct(shape2, F32)],
            in_specs=[pl.BlockSpec(memory_space=pltpu.VMEM)] * 4,
            out_specs=[any_space] * 2,
            scratch_shapes=[pltpu.VMEM((LAST_ROWS[-1], dim), F32), pltpu.SemaphoreType.DMA((2, layers + 1))],
            compiler_params=pltpu.CompilerParams(vmem_limit_bytes=30_000_000),
        )(sums[0], sums[1], sums[4], sums[5])
        return new_in[None, None], new_out[None, None]

    block_spec = P("row", "col")
    return jax.shard_map(device_program, mesh=mesh,
                         in_specs=(block_spec, block_spec, block_spec, block_spec),
                         out_specs=(block_spec, block_spec), check_vma=False)
```
